32 devices in a mesh: dep: 4 (over z), col: 2 (over y), row: 4 (over x, core).
Axes of the slice: x: 2, y: 2, z: 4, core: 2. Of those that a mesh axis runs over, the one named last changes fastest.
Arguments:
- x_tok: bfloat16 [16384, 2048], P(('dep', 'row'), 'col')
- w_up: bfloat16 [2048, 8192], P('row', 'col')
- w_down: bfloat16 [8192, 2048], P('row', 'col')
- grad_out: bfloat16 [16384, 2048], P(('dep', 'row'), 'col')
Outputs:
- output 1: bfloat16 [16384, 2048], P(('dep', 'row'), 'col')
- output 2: bfloat16 [16384, 2048], P(('dep', 'row'), 'col')
- output 3: float32 [2048, 8192], P(('row', 'dep'), 'col')
- output 4: float32 [8192, 2048], P(('row', 'dep'), 'col')
All inputs are finite; a program needn't handle non-finite values.
Results may differ from the reference program's by a relative error of at most 0.00118.
Values are sent between devices in bfloat16 or wider.
A program may use at most 1 GiB of HBM per device.

```python
import math
import jax
import jax.numpy as jnp
from jax import lax

HIDDEN = 2048
FFN_DIM = 8192
TOKENS = 16384

BLOCK_ROWS = math.gcd(TOKENS, 2048)
NUM_BLOCKS = TOKENS // BLOCK_ROWS
GELU_COEF = 0.7978845608028654
CUBIC_COEF = 0.044715


def gelu_fwd(pre_act):
    inner = GELU_COEF * (pre_act + CUBIC_COEF * pre_act * pre_act * pre_act)
    return 0.5 * pre_act * (1.0 + jnp.tanh(inner))


def gelu_slope(pre_act):
    inner = GELU_COEF * (pre_act + CUBIC_COEF * pre_act * pre_act * pre_act)
    tanh_val = jnp.tanh(inner)
    return 0.5 * (1.0 + tanh_val) + 0.5 * pre_act * (1.0 - tanh_val * tanh_val) * GELU_COEF * (1.0 + 3.0 * CUBIC_COEF * pre_act * pre_act)


def setup_inputs(seed: int = 0) -> dict:
    root_key = jax.random.key(seed)
    key_x, key_up, key_down, key_g = jax.random.split(root_key, 4)
    x_tok = jax.random.normal(key_x, (TOKENS, HIDDEN), jnp.float32).astype(jnp.bfloat16)
    w_up = (jax.random.normal(key_up, (HIDDEN, FFN_DIM), jnp.float32) * HIDDEN ** -0.5).astype(jnp.bfloat16)
    w_down = (jax.random.normal(key_down, (FFN_DIM, HIDDEN), jnp.float32) * FFN_DIM ** -0.5).astype(jnp.bfloat16)
    grad_out = jax.random.normal(key_g, (TOKENS, HIDDEN), jnp.float32).astype(jnp.bfloat16)
    return {"x_tok": x_tok, "w_up": w_up, "w_down": w_down, "grad_out": grad_out}


def reference(x_tok, w_up, w_down, grad_out):
    x_blocks = x_tok.reshape(NUM_BLOCKS, BLOCK_ROWS, HIDDEN)
    g_blocks = grad_out.reshape(NUM_BLOCKS, BLOCK_ROWS, HIDDEN)

    def block_step(acc_pair, block_in):
        dw_up_acc, dw_down_acc = acc_pair
        x_blk, g_blk = block_in
        pre_act = jnp.dot(x_blk, w_up, preferred_element_type=jnp.float32)
        hidden_act = gelu_fwd(pre_act).astype(jnp.bfloat16)
        y_blk = jnp.dot(hidden_act, w_down, preferred_element_type=jnp.float32).astype(jnp.bfloat16)
        d_act = jnp.dot(g_blk, w_down.T, preferred_element_type=jnp.float32)
        d_pre = (d_act * gelu_slope(pre_act)).astype(jnp.bfloat16)
        dx_blk = jnp.dot(d_pre, w_up.T, preferred_element_type=jnp.float32).astype(jnp.bfloat16)
        dw_up_acc = dw_up_acc + jnp.dot(x_blk.T, d_pre, preferred_element_type=jnp.float32)
        dw_down_acc = dw_down_acc + jnp.dot(hidden_act.T, g_blk, preferred_element_type=jnp.float32)
        return (dw_up_acc, dw_down_acc), (y_blk, dx_blk)

    init_acc = (jnp.zeros((HIDDEN, FFN_DIM), jnp.float32), jnp.zeros((FFN_DIM, HIDDEN), jnp.float32))
    (dw_up, dw_down), (y_blocks, dx_blocks) = lax.scan(block_step, init_acc, (x_blocks, g_blocks))
    return y_blocks.reshape(TOKENS, HIDDEN), dx_blocks.reshape(TOKENS, HIDDEN), dw_up, dw_down
```

```python
import jax
import jax.numpy as jnp
from jax import lax
from jax.sharding import PartitionSpec as P

GELU_COEF = 0.7978845608028654
CUBIC_COEF = 0.044715
NF = 2


def gelu_fwd(pre_act):
    inner = GELU_COEF * (pre_act + CUBIC_COEF * pre_act * pre_act * pre_act)
    return 0.5 * pre_act * (1.0 + jnp.tanh(inner))


def gelu_slope(pre_act):
    inner = GELU_COEF * (pre_act + CUBIC_COEF * pre_act * pre_act * pre_act)
    tanh_val = jnp.tanh(inner)
    return 0.5 * (1.0 + tanh_val) + 0.5 * pre_act * (1.0 - tanh_val * tanh_val) * GELU_COEF * (1.0 + 3.0 * CUBIC_COEF * pre_act * pre_act)


def dot(a, b, dims):
    return lax.dot_general(a, b, (dims, ((), ())), preferred_element_type=jnp.float32)


NN = ((1,), (0,))
NT = ((1,), (1,))
TN = ((0,), (0,))


def ordered(flag, own, other, axis):
    return jnp.where(flag == 0, jnp.concatenate([own, other], axis), jnp.concatenate([other, own], axis))


def after(value, *firsts):
    return lax.optimization_barrier((value, *(f[:1, :1] for f in firsts)))[0]


def dep_sum(v, axis):
    return lax.psum_scatter(v, "dep", scatter_dimension=axis, tiled=True)


def solution(mesh):
    act_spec = P(("dep", "row"), "col")
    wgt_spec = P("row", "col")
    grad_spec = P(("row", "dep"), "col")
    n_dep = mesh.shape["dep"]

    core_swap = [(r, r ^ 1) for r in range(4)]
    x_swap = [(r, r ^ 2) for r in range(4)]
    diag_swap = [(r, r ^ 3) for r in range(4)]
    y_swap = [(0, 1), (1, 0)]

    def plane(x, y, c):
        return y * 4 + x * 2 + c

    cells = [(x, y, c) for x in range(2) for y in range(2) for c in range(2)]
    to_w1 = [(plane(a, b, c), plane(b, a, c)) for a, b, c in cells]
    to_w2 = [(plane(a, b, c), plane(1 - b, a, c)) for a, b, c in cells]
    home_1 = [(plane(x, y, c), plane(y, x, c)) for x, y, c in cells]
    home_2 = [(plane(x, y, c), plane(y, 1 - x, c)) for x, y, c in cells]
    plane_axes = ("col", "row")

    def local_block(x_loc, w_up_loc, w_down_loc, g_loc):
        row = lax.axis_index("row")
        x, c = row // 2, row % 2
        y = lax.axis_index("col")
        tok, half = x_loc.shape
        rows_up = w_up_loc.shape[0]
        quarter = w_up_loc.shape[1] // 2
        sub = quarter // (n_dep * NF)
        chunk = quarter // NF

        x_in = lax.ppermute(x_loc, "col", y_swap)
        g_in = lax.ppermute(g_loc, "col", y_swap)
        w5 = w_up_loc.reshape(rows_up, 2, n_dep, NF, sub)
        w4 = w_down_loc.reshape(n_dep, NF, sub, half)
        up_in, down_in = [], []
        for j in range(NF):
            mine, theirs = (
                lax.dynamic_index_in_dim(w5, core, 1, keepdims=False)[:, :, j].reshape(rows_up, chunk) for core in (c, 1 - c)
            )
            near = lax.ppermute(theirs, "row", core_swap)
            far_same = lax.ppermute(mine, "row", x_swap)
            far_other = lax.ppermute(theirs, "row", diag_swap)
            up_in.append((mine, near, far_same, far_other))
        for j in range(NF):
            piece = w4[:, j].reshape(chunk, half)
            down_in.append((lax.ppermute(piece, plane_axes, to_w1), lax.ppermute(piece, plane_axes, to_w2)))

        def gather_tokens(v, v_in):
            v_row = ordered(y, v, v_in, 1)
            return jnp.concatenate([v_row, lax.ppermute(v_row, "row", core_swap)], 0)

        x_tok = gather_tokens(x_loc, x_in)
        g_tok = gather_tokens(g_loc, g_in)

        w_up = []
        for mine, near, far_same, far_other in up_in:
            w_up.append(ordered(x, ordered(c, mine, near, 0), ordered(c, far_same, far_other, 0), 0))
        pre = [dot(x_tok, w_up[j], NN) for j in range(NF)]
        hidden = [gelu_fwd(u).astype(jnp.bfloat16) for u in pre]

        part_down = [dot(hidden[j], g_tok, TN) for j in range(NF)]
        dw_down = [dep_sum(part_down[j], 0) for j in range(NF)]

        w_down = [ordered(x, *(after(v, *part_down) for v in down_in[j]), 1) for j in range(NF)]
        d_pre = []
        for j in range(NF):
            d_act = dot(g_tok, w_down[j], NT)
            d_pre.append((d_act * gelu_slope(pre[j])).astype(jnp.bfloat16))

        x_keep = lax.dynamic_slice_in_dim(x_tok, x * half, half, 1)
        x_send = lax.dynamic_slice_in_dim(x_tok, (1 - x) * half, half, 1)
        up_sent = [lax.ppermute(dot(x_send, d_pre[j], TN), "row", x_swap) for j in range(NF)]

        def token_sum(lhs, rhs_of, dims):
            near, far = rhs_of(y), rhs_of(1 - y)

            def part(tokens, rhs):
                out = dot(lhs[0][tokens], rhs[0], dims)
                for j in range(1, NF):
                    out = out + dot(lhs[j][tokens], rhs[j], dims)
                return out

            own, oth = slice(0, tok), slice(tok, 2 * tok)
            far_in = lax.ppermute(part(oth, far), "row", core_swap)
            near_in = lax.ppermute(part(oth, near), "row", core_swap)
            far_sum = part(own, far) + far_in
            far_y = lax.ppermute(far_sum, "col", y_swap)
            return far_sum, far_y, part(own, near) + near_in

        _, y_in, y_near = token_sum(hidden, lambda k: [lax.dynamic_slice_in_dim(w, k * half, half, 1) for w in w_down], NN)
        _, d_in, d_near = token_sum(d_pre, lambda k: [lax.dynamic_slice_in_dim(w, k * half, half, 0) for w in w_up], NT)

        dw_up = []
        for j in range(NF):
            sent = after(up_sent[j], y_near, d_near)
            part = (dot(x_keep, d_pre[j], TN) + sent).reshape(2, half // 2, chunk)
            dw_up.append(dep_sum(part, 1))

        y_out = (y_near + y_in).astype(jnp.bfloat16)
        dx_out = (d_near + d_in).astype(jnp.bfloat16)

        down_parts = []
        for j in range(NF):
            a = lax.dynamic_slice_in_dim(dw_down[j], x * half, half, 1)
            b = lax.dynamic_slice_in_dim(dw_down[j], (1 - x) * half, half, 1)
            down_parts.append(lax.ppermute(a, plane_axes, home_1) + lax.ppermute(b, plane_axes, home_2))
        dw_down_out = jnp.concatenate(down_parts, 0)

        up_parts = []
        for j in range(NF):
            mine = lax.dynamic_index_in_dim(dw_up[j], c, 0, keepdims=False)
            theirs = lax.dynamic_index_in_dim(dw_up[j], 1 - c, 0, keepdims=False)
            other = lax.ppermute(theirs, "row", core_swap)
            up_parts.append(ordered(c, mine[:, None], other[:, None], 1).reshape(mine.shape[0], 2, n_dep, 1, sub))
        dw_up_out = jnp.concatenate(up_parts, 3).reshape(up_parts[0].shape[0], 2 * quarter)
        return y_out, dx_out, dw_up_out, dw_down_out

    return jax.shard_map(local_block, mesh=mesh, in_specs=(act_spec, wgt_spec, wgt_spec, act_spec), out_specs=(act_spec, act_spec, grad_spec, grad_spec), check_vma=False)
```

```python
import jax
import jax.numpy as jnp
from jax import lax
from jax.experimental import pallas as pl
from jax.experimental.pallas import tpu as pltpu
from jax.sharding import PartitionSpec as P

GELU_COEF = 0.7978845608028654
CUBIC_COEF = 0.044715


def gelu_fwd(pre_act):
    inner = GELU_COEF * (pre_act + CUBIC_COEF * pre_act * pre_act * pre_act)
    return 0.5 * pre_act * (1.0 + jnp.tanh(inner))


def gelu_slope(pre_act):
    inner = GELU_COEF * (pre_act + CUBIC_COEF * pre_act * pre_act * pre_act)
    tanh_val = jnp.tanh(inner)
    return 0.5 * (1.0 + tanh_val) + 0.5 * pre_act * (1.0 - tanh_val * tanh_val) * GELU_COEF * (1.0 + 3.0 * CUBIC_COEF * pre_act * pre_act)


NN = ((1,), (0,))
NT = ((1,), (1,))
TN = ((0,), (0,))


def dot(a, b, dims, plus=None):
    out = lax.dot_general(a, b, (dims, ((), ())), preferred_element_type=jnp.float32)
    return out if plus is None else out + plus


def ordered(flag, own, other, axis):
    return jnp.where(flag == 0, jnp.concatenate([own, other], axis), jnp.concatenate([other, own], axis))


def whole(value):
    return lax.optimization_barrier(value)


def dep_sum(v):
    return lax.psum_scatter(v, "dep", scatter_dimension=0, tiled=True)


ANY = pl.BlockSpec(memory_space=pl.ANY)


def place(refs, target, places, sems):
    copies = []
    for i, (ref, (r, c)) in enumerate(zip(refs, places)):
        rows, cols = ref.shape
        spot = target.at[pl.ds(pl.multiple_of(r, rows), rows), pl.ds(pl.multiple_of(c, cols), cols)]
        copies.append(pltpu.make_async_copy(ref, spot, sems.at[i]))
        copies[-1].start()
    return copies


def assemble(pieces, places_of, shape):
    def kernel(*refs):
        srcs, out, buf, sem_in, sem_out = refs[: len(pieces)], *refs[len(pieces) :]
        places = places_of()
        copies = place(srcs, buf, places, sem_in)
        outs = []
        for i, (ref, (r, c)) in enumerate(zip(srcs, places)):
            rows, cols = ref.shape
            spot = (pl.ds(pl.multiple_of(r, rows), rows), pl.ds(pl.multiple_of(c, cols), cols))
            copies[i].wait()
            outs.append(pltpu.make_async_copy(buf.at[spot], out.at[spot], sem_out.at[i]))
            outs[-1].start()
        for o in outs:
            o.wait()

    n = len(pieces)
    return pl.pallas_call(
        kernel,
        out_shape=jax.ShapeDtypeStruct(shape, pieces[0].dtype),
        in_specs=[ANY] * n,
        out_specs=ANY,
        scratch_shapes=[pltpu.VMEM(shape, pieces[0].dtype), pltpu.SemaphoreType.DMA((n,)), pltpu.SemaphoreType.DMA((n,))],
        compiler_params=pltpu.CompilerParams(vmem_limit_bytes=24 * 2**20),
        cost_estimate=pl.CostEstimate(flops=10**8, bytes_accessed=4 * shape[0] * shape[1], transcendentals=0),
    )(*pieces)


def up_product(x_pieces, x_places_of, w_pieces, w_places_of, tokens, hid, feats):
    nx, nw = len(x_pieces), len(w_pieces)
    tile_n, tile_m = min(256, feats), min(512, tokens)

    def kernel(*refs):
        xs, ws, (x_out, w_out, u_out, a_out, x_buf, w_buf, sem_x, sem_w, sem_out) = refs[:nx], refs[nx : nx + nw], refs[nx + nw :]
        step = pl.program_id(0)

        @pl.when(step == 0)
        def _():
            copies = place(xs, x_buf, x_places_of(), sem_x) + place(ws, w_buf, w_places_of(), sem_w)
            for copy in copies:
                copy.wait()
            pltpu.make_async_copy(x_buf, x_out, sem_out.at[0]).start()
            pltpu.make_async_copy(w_buf, w_out, sem_out.at[1]).start()

        w_tile = w_buf[:, pl.ds(pl.multiple_of(step * tile_n, tile_n), tile_n)]

        @pl.loop(0, tokens // tile_m)
        def _(m):
            rows = pl.ds(pl.multiple_of(m * tile_m, tile_m), tile_m)
            u = jnp.dot(x_buf[rows, :], w_tile, preferred_element_type=jnp.float32)
            u_out[rows, :] = u
            a_out[rows, :] = gelu_fwd(u).astype(jnp.bfloat16)

        @pl.when(step == feats // tile_n - 1)
        def _():
            pltpu.make_async_copy(x_buf, x_out, sem_out.at[0]).wait()
            pltpu.make_async_copy(w_buf, w_out, sem_out.at[1]).wait()

    tile = pl.BlockSpec((tokens, tile_n), lambda i: (0, i))
    return pl.pallas_call(
        kernel,
        grid=(feats // tile_n,),
        out_shape=(
            jax.ShapeDtypeStruct((tokens, hid), jnp.bfloat16),
            jax.ShapeDtypeStruct((hid, feats), jnp.bfloat16),
            jax.ShapeDtypeStruct((tokens, feats), jnp.float32),
            jax.ShapeDtypeStruct((tokens, feats), jnp.bfloat16),
        ),
        in_specs=[ANY] * (nx + nw),
        out_specs=(ANY, ANY, tile, tile),
        scratch_shapes=[
            pltpu.VMEM((tokens, hid), jnp.bfloat16),
            pltpu.VMEM((hid, feats), jnp.bfloat16),
            pltpu.SemaphoreType.DMA((nx,)),
            pltpu.SemaphoreType.DMA((nw,)),
            pltpu.SemaphoreType.DMA((2,)),
        ],
        compiler_params=pltpu.CompilerParams(vmem_limit_bytes=40 * 2**20, dimension_semantics=("arbitrary",)),
        cost_estimate=pl.CostEstimate(flops=2 * tokens * hid * feats, bytes_accessed=10 * tokens * feats, transcendentals=tokens * feats),
        name="up_product",
    )(*x_pieces, *w_pieces)


def solution(mesh):
    act_spec = P(("dep", "row"), "col")
    wgt_spec = P("row", "col")
    grad_spec = P(("row", "dep"), "col")
    n_dep = mesh.shape["dep"]

    core_swap = [(r, r ^ 1) for r in range(4)]
    x_swap = [(r, r ^ 2) for r in range(4)]
    diag_swap = [(r, r ^ 3) for r in range(4)]
    y_swap = [(0, 1), (1, 0)]

    def plane(x, y, c):
        return y * 4 + x * 2 + c

    cells = [(x, y, c) for x in range(2) for y in range(2) for c in range(2)]
    to_w1 = [(plane(a, b, c), plane(b, a, c)) for a, b, c in cells if a != b]
    to_w2 = [(plane(a, b, c), plane(1 - b, a, c)) for a, b, c in cells]
    home_near = [(plane(1 - y, y, c), plane(y, y, c)) for x, y, c in cells if x == 0]
    home_side = [(plane(y, y, c), plane(y, 1 - y, c)) for x, y, c in cells if x == 0]
    home_diag = [(plane(1 - y, y, c), plane(y, 1 - y, c)) for x, y, c in cells if x == 0]
    plane_axes = ("col", "row")

    def local_block(x_loc, w_up_loc, w_down_loc, g_loc):
        row = lax.axis_index("row")
        x, c = row // 2, row % 2
        y = lax.axis_index("col")
        z = lax.axis_index("dep")
        tok, half = x_loc.shape
        rows_up = w_up_loc.shape[0]
        quarter = w_up_loc.shape[1] // 2
        same = x == y

        x_in = lax.ppermute(x_loc, "col", y_swap)
        share = rows_up // n_dep
        part = quarter // 2

        def up_piece(core, j, start=0, rows=rows_up):
            return lax.dynamic_slice(w_up_loc, (start, core * quarter + j * part), (rows, part))

        far_q = jnp.stack(
            [
                lax.ppermute(up_piece(c, 1, z * share, share), "row", x_swap),
                lax.ppermute(up_piece(1 - c, 1, z * share, share), "row", diag_swap),
            ]
        )
        far_up = [lax.ppermute(up_piece(c, 0), "row", x_swap), lax.ppermute(up_piece(1 - c, 0), "row", diag_swap)]
        g_in = lax.ppermute(g_loc, "col", y_swap)
        x_core = lax.ppermute(x_loc, "row", core_swap)
        g_core = lax.ppermute(g_loc, "row", core_swap)
        near_up = lax.ppermute(lax.dynamic_slice_in_dim(w_up_loc, (1 - c) * quarter, quarter, 1), "row", core_swap)
        at_x = lax.ppermute(w_down_loc, plane_axes, to_w1)
        at_nx = lax.ppermute(w_down_loc, plane_axes, to_w2)
        far_q = lax.all_gather(far_q, "dep", axis=1, tiled=True)
        x_in_core = lax.ppermute(x_in, "row", core_swap)
        g_own = whole(jnp.concatenate([g_loc, g_core], 0))
        mine = lax.dynamic_slice_in_dim(w_up_loc, c * quarter, quarter, 1)

        def position():
            row = lax.axis_index("row")
            return row // 2, row % 2, lax.axis_index("col")

        def x_places():
            return ((0, 0), (0, half), (tok, 0), (tok, half))

        def w_places():
            x, c, y = position()
            near, far = (x ^ y) * half, (1 - (x ^ y)) * half
            own, oth = c * rows_up, (1 - c) * rows_up
            return ((near + own, 0), (near + oth, 0), (far + own, 0), (far + oth, 0), (far + own, part), (far + oth, part))

        x_tok, w_up, pre, hidden = up_product(
            (x_loc, x_in, x_core, x_in_core), x_places, (mine, near_up, *far_up, far_q[0], far_q[1]), w_places, 2 * tok, 2 * half, quarter
        )

        own = dep_sum(dot(hidden, g_own, TN))

        g_in_core = lax.ppermute(g_in, "row", core_swap)
        g_tok = assemble((g_loc, g_in, g_core, g_in_core), x_places, (2 * tok, 2 * half))
        quart = half // 2

        def oth_cols(side):
            return lax.dynamic_slice_in_dim(g_tok, half + side * quart, quart, 1)

        oth_in = lax.ppermute(dot(hidden, oth_cols(1 - x), TN), "row", x_swap)

        def dn_places():
            x, _, y = position()
            return ((0, (x ^ y) * half), (0, (1 - (x ^ y)) * half))

        at_x = jnp.where(same, w_down_loc, at_x)
        w_down = assemble((at_x, at_nx), dn_places, (quarter, 2 * half))

        def block_cols(rows_x, e):
            core = c if e else 1 - c
            return lax.dynamic_slice_in_dim(x_tok, ((rows_x ^ y) * 2 + core) * rows_up, rows_up, 1)

        d_act = dot(g_tok, w_down, NT)
        d_pre = (d_act * gelu_slope(pre)).astype(jnp.bfloat16)
        dw_in = [lax.ppermute(dot(block_cols(1 - x, e), d_pre, TN), "row", x_swap) for e in range(2)]

        own_tok, oth_tok = slice(0, tok), slice(tok, 2 * tok)

        def token_sum(lhs, rhs_own, rhs_oth, dims):
            far_core = lax.ppermute(dot(lhs[oth_tok], rhs_oth, dims), "row", core_swap)
            near_core = lax.ppermute(dot(lhs[oth_tok], rhs_own, dims), "row", core_swap)
            far = lax.ppermute(dot(lhs[own_tok], rhs_oth, dims, far_core), "col", y_swap)
            return dot(lhs[own_tok], rhs_own, dims, near_core + far).astype(jnp.bfloat16)

        y_out = token_sum(hidden, w_down[:, :half], w_down[:, half:], NN)
        dx_out = token_sum(d_pre, w_up[:half], w_up[half:], NT)

        oth = dep_sum(dot(hidden, oth_cols(x), TN, oth_in))
        dw_up = [dep_sum(dot(block_cols(x, e), d_pre, TN, dw_in[e])) for e in range(2)]

        near = own + lax.ppermute(own, plane_axes, home_near)
        side = lax.ppermute(oth, plane_axes, home_side)
        diag = lax.ppermute(oth, plane_axes, home_diag)
        dw_down_out = jnp.where(same, near, ordered(x, side, diag, 1))
        dw_up_out = ordered(c, dw_up[1], lax.ppermute(dw_up[0], "row", core_swap), 1)
        return y_out, dx_out, dw_up_out, dw_down_out

    return jax.shard_map(local_block, mesh=mesh, in_specs=(act_spec, wgt_spec, wgt_spec, act_spec), out_specs=(act_spec, act_spec, grad_spec, grad_spec), check_vma=False)
```
